1024 devices in a mesh: vb: 32 (over x, z_lo), vc: 32 (over z_hi, y, core).
Axes of the slice: x: 4, y: 8, z: 16 (z_hi: 2, z_lo: 8; z = z_hi * 8 + z_lo), core: 2. Of those that a mesh axis runs over, the one named last changes fastest.
Arguments:
- integrals: float32 [2, 512, 512, 512], P(None, 'vb', 'vc'), may hold values from -0.25 to 0.25
- doubles: float32 [3, 512, 512], P(None, 'vb'), may hold values from -6 to 6
- eps_occ: float32 [100], replicated, may hold values from -2 to -0.5
- eps_virt: float32 [512], replicated, may hold values from 0.2 to 3
- triple: int32 [3], replicated, may hold values from 0 to 99
- energy_order: int32 [512], replicated, may hold values from 0 to 511, each once
Outputs:
- amplitudes: float32 [512, 512, 512], P('vb', 'vc')
- grad: float32 [512, 512], P('vb', 'vc')
The draws below stay inside these ranges and needn't reach their ends.
Inputs may be any that keep to these rules, and one draw needn't show every extreme that they name: `energy_order`: each of 0 to 511 appears once.
All inputs are finite; a program needn't handle non-finite values.
Results may differ from the reference program's by a relative error of at most 0.00007.
Values sent between devices are 32-bit elements; how exact they have to be, the bound alone decides.
A program may use at most 64 MiB of HBM per device.

```python
import jax
import jax.numpy as jnp
from jax import lax

V = 512
NOCC = 100


def shard_levels(own_key, extent, pieces, smallest, high):
    factor_of = 1.0
    for dim, shards_of in pieces:
        heights = jax.random.uniform(jax.random.fold_in(jax.random.fold_in(own_key, 6), dim), (shards_of,), jnp.float32, smallest / len(pieces), high / len(pieces))
        factor_of = factor_of * jnp.repeat(jnp.exp(heights), extent[dim] // shards_of).reshape((-1,) + (1,) * (len(extent) - 1 - dim))
    return factor_of


def normal_values(own_key, extent, scale, limit, cuts=(), kind=jnp.bfloat16):
    values = scale * jax.random.normal(own_key, extent, jnp.float32)
    if cuts:
        values = values * shard_levels(own_key, extent, cuts, -0.22, 0.18)
    return jnp.clip(values, -limit, limit).astype(kind)


def setup_inputs(seed: int = 0) -> dict:
    key_list = jax.random.split(jax.random.key(seed), 7)
    integrals = normal_values(key_list[0], (2, V, V, V), V ** -0.5, 0.25, ((1, 32), (2, 32)), jnp.float32)
    doubles = normal_values(key_list[1], (3, V, V), 1.0, 6.0, ((1, 32),), jnp.float32)
    eps_occ = jnp.clip(jax.random.uniform(key_list[2], (NOCC,), jnp.float32, -2.0, -0.5), -2.0, -0.5)
    eps_virt = jnp.clip(jax.random.uniform(key_list[3], (V,), jnp.float32, 0.2, 3.0), 0.2, 3.0)
    triple = jax.random.randint(key_list[4], (3,), 0, NOCC).astype(jnp.int32)
    energy_order = jax.random.permutation(key_list[5], V).astype(jnp.int32)
    return {"integrals": integrals, "doubles": doubles, "eps_occ": eps_occ, "eps_virt": eps_virt, "triple": triple, "energy_order": energy_order}


def reference(integrals, doubles, eps_occ, eps_virt, triple, energy_order):
    highest = lax.Precision.HIGHEST
    k_block = integrals[0]
    i_block = integrals[1]
    first_term = jnp.einsum('bcd,ad->bca', k_block, doubles[0], precision=highest)
    second_term = jnp.einsum('acd,bd->bca', k_block, doubles[1], precision=highest)
    third_term = jnp.einsum('bad,cd->bca', i_block, doubles[2], precision=highest)
    positions = jnp.arange(V, dtype=jnp.int32)
    one_hot = energy_order[:, None] == positions[None, :]
    virt_energy = jnp.sum(jnp.where(one_hot, eps_virt[None, :], jnp.float32(0.0)), axis=1)
    occ_positions = jnp.arange(NOCC, dtype=jnp.int32)
    occ_hot = triple[:, None] == occ_positions[None, :]
    occ_energy = jnp.sum(jnp.where(occ_hot, eps_occ[None, :], jnp.float32(0.0)))
    denominator = occ_energy - virt_energy[:, None, None] - virt_energy[None, :, None] - virt_energy[None, None, :]
    amplitudes = (first_term + second_term + third_term) / denominator
    grad = jnp.einsum('bca,bcd->ad', amplitudes, k_block, precision=highest)
    return amplitudes, grad
```

```python
import jax
import jax.numpy as jnp
from jax import lax
from jax.experimental import pallas as pl
from jax.experimental.pallas import tpu as pltpu
from jax.sharding import PartitionSpec as P

V = 512
NOCC = 100
MESH = pl.DeviceIdType.MESH
F32 = jnp.float32
BF16 = jnp.bfloat16
NT = (((1,), (1,)), ((), ()))
NN = (((1,), (0,)), ((), ()))


def halves(x):
    high = x.astype(BF16)
    return high, (x - high.astype(F32)).astype(BF16)


def dot3(ah, al, bh, bl, dims):
    def one(a, b):
        return lax.dot_general(a, b, dims, preferred_element_type=F32)

    return one(ah, bh) + (one(ah, bl) + one(al, bh))


def swap_granules(xs, lane):
    xs = list(xs)
    for s in (1, 2, 4):
        upper = (lane & (16 * s)) != 0
        for i in range(8):
            if i & s == 0:
                a, b = xs[i], xs[i + s]
                xs[i] = jnp.where(upper, pltpu.roll(b, 16 * s, 1), a)
                xs[i + s] = jnp.where(upper, b, pltpu.roll(a, 128 - 16 * s, 1))
    return xs


def kernel(
    ints, dbl, eps_occ, eps_virt, triple, order, amp_out, grad_out,
    kf, fi, g_all, kh, kl, ph, plo, ih, il, s2, s3, r2, r3, t2, first, amp, ev, eb,
    part, c0, q0, xr, q1, yr, q2, zr, q3, fr,
    load_sem, zs, zr_sem, ys, yr_sem, xs, xr_sem, cs, cr_sem, as2, ar2, as3, ar3, out_sem,
    ps, pr, gxs, gxr, gys, gyr, gzs, gzr, gfs, gfr,
):
    vb = lax.axis_index("vb")
    vc = lax.axis_index("vc")
    x, z = vb // 8, vb % 8
    h, y, k = vc // 16, (vc // 2) % 8, vc % 2
    other = 1 - k

    def dev(x_=x, z_=z, h_=h, y_=y, k_=k):
        return (x_ * 8 + z_, h_ * 16 + y_ * 2 + k_)

    def send(src, dst, s_sem, r_sem, to):
        pltpu.make_async_remote_copy(
            src_ref=src, dst_ref=dst, send_sem=s_sem, recv_sem=r_sem, device_id=to, device_id_type=MESH
        ).start()

    def drain(ref, sem):
        pltpu.make_async_copy(ref, ref, sem).wait()

    loads = []
    for l in range(4):
        loads.append(pltpu.make_async_copy(ints.at[0, :, pl.ds(128 * l, 128)], kf.at[l], load_sem.at[1]))
        loads.append(pltpu.make_async_copy(ints.at[1, :, pl.ds(128 * l, 128)], fi.at[l], load_sem.at[2]))
    yt, yl = y // 4, y % 4
    mine = z // 4 == k

    @pl.when(mine)
    def _():
        rows = pl.ds(pl.multiple_of(8 * yt, 8), 8)
        cols = pl.ds(pl.multiple_of(128 * yl, 128), 128)
        for m in range(3):
            pltpu.make_async_copy(dbl.at[m, rows, cols], g_all.at[m, vb, yt, yl], load_sem.at[0]).start()

    for copy in loads:
        copy.start()

    barrier = pltpu.get_barrier_semaphore()

    def greet(j, carry):
        pl.semaphore_signal(barrier, inc=1, device_id=((vb + j) % 32, vc), device_id_type=MESH)
        pl.semaphore_signal(barrier, inc=1, device_id=(vb, (vc + j) % 32), device_id_type=MESH)
        return carry

    lax.fori_loop(1, 32, greet, 0)
    for j in range(1, 8):
        pl.semaphore_signal(
            barrier, inc=1, device_id=dev(z_=(z + j) % 8, h_=1 - h), device_id_type=MESH
        )
    pl.semaphore_wait(barrier, 69)

    @pl.when(mine)
    def _():
        drain(g_all.at[0:3, vb, yt, yl], load_sem.at[0])
        for m in (2, 1, 0):
            for j in range(1, 8):
                send(
                    g_all.at[m, vb, yt, yl], g_all.at[m, vb, yt, yl],
                    zs.at[m], zr_sem.at[m], dev(z_=(z + j) % 8),
                )

    drain(kf, load_sem.at[1])
    for l in range(4):
        cols = pl.ds(128 * l, 128)
        high, low = halves(kf[l])
        kh[:, cols] = high
        kl[:, cols] = low
        for c in range(16):
            high, low = halves(kf[l, pl.ds(c, 16, stride=16), :])
            ph[pl.ds(16 * c, 16), cols] = high
            plo[pl.ds(16 * c, 16), cols] = low
    drain(fi, load_sem.at[2])
    for l in range(4):
        cols = pl.ds(128 * l, 128)
        high, low = halves(fi[l])
        ih[:, cols] = high
        il[:, cols] = low

    half = 8 * x + 4 * k
    for m in (2, 1, 0):
        @pl.when(mine)
        def _():
            drain(g_all.at[m, 0, 0, pl.ds(0, 3)], zr_sem.at[m])

        @pl.when(jnp.logical_not(mine))
        def _():
            drain(g_all.at[m, 0, 0], zr_sem.at[m])

        block = g_all.at[m, pl.ds(half, 4), yt, yl]
        for j in range(1, 8):
            send(block, block, ys.at[m], yr_sem.at[m], dev(y_=(y + j) % 8))

    for m in (2, 1, 0):
        drain(g_all.at[0, pl.ds(0, 7), 0], yr_sem.at[m])
        block = g_all.at[m, pl.ds(half, 4)]
        for j in (1, 3, 2):
            send(block, block, xs.at[m], xr_sem.at[m, x], dev(x_=(x + j) % 4))
        send(block, block, cs.at[m], cr_sem.at[m, x], dev(k_=other))

    def rows_of(m, j):
        xg = (x + j) % 4
        if j:
            block = g_all.at[m, pl.ds(8 * xg + 4 * k, 4)]
            drain(block, xr_sem.at[m, xg])
            send(block, block, cs.at[m], cr_sem.at[m, xg], dev(k_=other))
        drain(g_all.at[m, pl.ds(8 * xg + 4 * other, 4)], cr_sem.at[m, xg])
        tiles = g_all.at[m, pl.ds(8 * xg, 8)]
        high, low = halves(
            jnp.concatenate([tiles[:, :, l].reshape(128, 128) for l in range(4)], axis=1)
        )
        return xg, high, low

    for j in (0, 1, 3, 2):
        xg, dh, dl = rows_of(2, j)
        s3[pl.ds(8 * xg, 8)] = dot3(dh, dl, ih[...], il[...], NT).reshape(8, 16, 256)

        def give(i, carry):
            to = 8 * xg + i

            @pl.when(to == vc)
            def _():
                r3[vc] = s3[vc]

            @pl.when(to != vc)
            def _():
                send(s3.at[to], r3.at[vc], as3, ar3, (vb, to))

            return carry

        lax.fori_loop(0, 8, give, 0)

    for j in (0, 1, 3, 2):
        xg, dh, dl = rows_of(1, j)
        s2[pl.ds(8 * xg, 8)] = dot3(dh, dl, ph[...], plo[...], NT).reshape(8, 16, 256)

        def give(i, carry):
            to = 8 * xg + i

            @pl.when(to == vb)
            def _():
                r2[vb] = s2[vb]

            @pl.when(to != vb)
            def _():
                send(s2.at[to], r2.at[vb], as2, ar2, (to, vc))

            return carry

        lax.fori_loop(0, 8, give, 0)

    for j in (0, 1, 3, 2):
        xg, dh, dl = rows_of(0, j)
        first[xg] = dot3(kh[...], kl[...], dh, dl, NT)

    hot = lax.broadcasted_iota(jnp.int32, (V, V), 0) == order[...]
    e_high, e_low = halves(jnp.broadcast_to(eps_virt[...], (8, V)))
    e_rest = (jnp.broadcast_to(eps_virt[...], (8, V)) - e_high.astype(F32) - e_low.astype(F32)).astype(BF16)
    hot = jnp.where(hot, F32(1.0), F32(0.0)).astype(BF16)
    energy = sum(lax.dot_general(e, hot, NN, preferred_element_type=F32) for e in (e_rest, e_low, e_high))[0:1]
    for l in range(4):
        ev[l] = energy[:, 128 * l : 128 * l + 128]
    row = lax.broadcasted_iota(jnp.int32, (256, V), 0)
    col = lax.broadcasted_iota(jnp.int32, (256, V), 1)
    picked = jnp.where(col == 16 * vb + row // 16, energy, F32(0.0))
    b_energy = jnp.sum(picked, axis=1, keepdims=True)
    picked = jnp.where(col == 16 * vc + row % 16, energy, F32(0.0))
    c_energy = jnp.sum(picked, axis=1, keepdims=True)
    occ = eps_occ[0, triple[0, 0]] + eps_occ[0, triple[0, 1]] + eps_occ[0, triple[0, 2]]
    eb[...] = jnp.broadcast_to(occ - b_energy - c_energy, (256, 128))

    drain(s3.at[pl.ds(0, 31)], ar3)
    drain(s2.at[pl.ds(0, 31)], ar2)

    lane = lax.broadcasted_iota(jnp.int32, (8, 128), 1)
    for j in (2, 1, 3, 0):
        g = (x + j) % 4
        for bt in range(2):
            for ch in range(2):
                ws = [r2[8 * g + i, 8 * bt : 8 * bt + 8, 128 * ch : 128 * ch + 128] for i in range(8)]
                for i, w in enumerate(swap_granules(ws, lane)):
                    t2[j, pl.ds(128 * bt + 8 * ch + i, 8, stride=16), :] = w
        for ct in range(2):
            for bh in range(2):
                ws = [r3[8 * g + i, 8 * ct : 8 * ct + 8, 128 * bh : 128 * bh + 128] for i in range(8)]
                for i, w in enumerate(swap_granules(ws, lane)):
                    at = pl.ds((8 * bh + i) * 16 + 8 * ct, 8)
                    first[g, at] = first[g, at] + w
        total = (first[g] + t2[j]) / (eb[...] - ev[g])
        amp[j] = total
        pltpu.make_async_copy(
            amp.at[j], amp_out.at[:, pl.ds(pl.multiple_of(128 * g, 128), 128)], out_sem
        ).start()
        th, tl = halves(total.T)
        part[pl.ds(8 * g, 8)] = dot3(th, tl, kh[...], kl[...], NN).reshape(8, 2, 8, V)
        send(part.at[pl.ds(8 * g, 8), other], c0.at[pl.ds(8 * g, 8)], ps, pr.at[g], dev(k_=other))

    for j in (2, 1, 3, 0):
        g = (x + j) % 4
        block = pl.ds(8 * g, 8)
        drain(c0.at[block], pr.at[g])
        q0[block] = part[block, k] + c0[block]
        if j:
            send(q0.at[block], xr.at[j - 1], gxs, gxr, dev(x_=g))
    drain(xr, gxr)
    q1[...] = (q0[pl.ds(8 * x, 8)] + xr[0]) + (xr[1] + xr[2])
    for j in range(1, 8):
        send(q1.at[(y + j) % 8], yr.at[j - 1], gys, gyr, dev(y_=(y + j) % 8))
    drain(yr, gyr)
    rows = q1[y] + jnp.sum(yr[...], axis=0)
    q2[0] = rows[:, 0:256]
    q2[1] = rows[:, 256:512]
    for hh in range(2):
        here = jnp.logical_and(z == y, h == hh)

        @pl.when(here)
        def _():
            zr[8 * h + z] = q2[hh]

        @pl.when(jnp.logical_not(here))
        def _():
            send(q2.at[hh], zr.at[8 * h + z], gzs.at[hh], gzr, dev(z_=y, h_=hh))

    @pl.when(z == y)
    def _():
        drain(zr.at[pl.ds(0, 15)], gzr)
        total = jnp.sum(zr[...], axis=0)
        q3[0] = total[:, 0:128]
        q3[1] = total[:, 128:256]

        def give(i, carry):
            @pl.when(16 * h + i == vc)
            def _():
                fr[k] = q3[i // 8]

            @pl.when(16 * h + i != vc)
            def _():
                send(q3.at[i // 8], fr.at[k], gfs, gfr.at[k], (vb, 16 * h + i))

            return carry

        lax.fori_loop(0, 16, give, 0)

    for r in range(2):
        @pl.when(jnp.logical_or(z != y, k != r))
        def _():
            drain(fr.at[r], gfr.at[r])

    place = vc % 8
    for r in range(2):
        got = fr[r]
        mine_cols = got[:, 0:16]
        for i in range(1, 8):
            mine_cols = jnp.where(place == i, got[:, 16 * i : 16 * i + 16], mine_cols)
        grad_out[8 * r : 8 * r + 8, :] = mine_cols

    @pl.when(mine)
    def _():
        for m in range(3):
            drain(g_all.at[m, pl.ds(0, 7), 0, 0], zs.at[m])

    for m in range(3):
        drain(g_all.at[0, pl.ds(0, 7), 0], ys.at[m])
        drain(g_all.at[m, pl.ds(0, 12)], xs.at[m])
        drain(g_all.at[m, pl.ds(0, 16)], cs.at[m])
    drain(s3.at[pl.ds(0, 31)], as3)
    drain(s2.at[pl.ds(0, 31)], as2)
    drain(c0, ps)
    drain(xr, gxs)
    drain(yr, gys)
    for hh in range(2):
        @pl.when(jnp.logical_not(jnp.logical_and(z == y, h == hh)))
        def _():
            drain(q2.at[hh], gzs.at[hh])

    @pl.when(z == y)
    def _():
        drain(t2.at[0, pl.ds(0, 120)], gfs)

    drain(amp, out_sem)


def on_device(integrals, doubles, eps_occ, eps_virt, triple, energy_order):
    vmem = pl.BlockSpec(memory_space=pltpu.VMEM)
    smem = pl.BlockSpec(memory_space=pltpu.SMEM)
    anyw = pl.BlockSpec(memory_space=pl.ANY)
    dma = pltpu.SemaphoreType.DMA
    f = lambda *s: pltpu.VMEM(s, F32)
    b = lambda *s: pltpu.VMEM(s, BF16)
    amp, grad = pl.pallas_call(
        kernel,
        out_shape=(jax.ShapeDtypeStruct((256, V), F32), jax.ShapeDtypeStruct((16, 16), F32)),
        in_specs=[anyw, anyw, smem, vmem, smem, vmem],
        out_specs=(anyw, vmem),
        scratch_shapes=[
            f(4, 256, 128), f(4, 256, 128), f(3, 32, 2, 4, 8, 128),
            b(256, V), b(256, V), b(256, V), b(256, V), b(256, V), b(256, V),
            f(32, 16, 256), f(32, 16, 256), f(32, 16, 256), f(32, 16, 256),
            f(4, 256, 128), f(4, 256, 128), f(4, 256, 128), f(4, 1, 128), f(256, 128),
            f(32, 2, 8, V), f(32, 8, V), f(32, 8, V), f(3, 8, 8, V), f(8, 8, V), f(7, 8, V),
            f(2, 8, 256), f(16, 8, 256), f(2, 8, 128), f(2, 8, 128),
            dma((3,)), dma((3,)), dma((3,)), dma((3,)), dma((3,)), dma((3,)), dma((3, 4)), dma((3,)), dma((3, 4)),
            dma, dma, dma, dma, dma,
            dma, dma((4,)), dma, dma, dma, dma, dma((2,)), dma, dma, dma((2,)),
        ],
        compiler_params=pltpu.CompilerParams(
            collective_id=0, has_side_effects=True, vmem_limit_bytes=48 * 1024 * 1024
        ),
    )(
        integrals.reshape(2, 256, V),
        doubles,
        eps_occ.reshape(1, NOCC),
        eps_virt.reshape(1, V),
        triple.reshape(1, 3),
        energy_order.reshape(1, V),
    )
    return amp.reshape(16, 16, V), grad


def solution(mesh):
    return jax.shard_map(
        on_device,
        mesh=mesh,
        in_specs=(P(None, "vb", "vc", None), P(None, "vb", None), P(), P(), P(), P()),
        out_specs=(P("vb", "vc", None), P("vb", "vc")),
        check_vma=False,
    )
```

```python
import jax
import jax.numpy as jnp
from jax import lax
from jax.experimental import pallas as pl
from jax.experimental.pallas import tpu as pltpu
from jax.sharding import PartitionSpec as P

V = 512
NOCC = 100
MESH = pl.DeviceIdType.MESH
F32 = jnp.float32
BF16 = jnp.bfloat16
NT = (((1,), (1,)), ((), ()))
NN = (((1,), (0,)), ((), ()))


def halves(x):
    high = x.astype(BF16)
    return high, (x - high.astype(F32)).astype(BF16)


def dot3(ah, al, bh, bl, dims):
    def one(a, b):
        return lax.dot_general(a, b, dims, preferred_element_type=F32)

    return one(ah, bh) + (one(ah, bl) + one(al, bh))


def swap_granules(xs, lane):
    xs = list(xs)
    for s in (1, 2, 4):
        upper = (lane & (16 * s)) != 0
        for i in range(8):
            if i & s == 0:
                a, b = xs[i], xs[i + s]
                xs[i] = jnp.where(upper, pltpu.roll(b, 16 * s, 1), a)
                xs[i + s] = jnp.where(upper, b, pltpu.roll(a, 128 - 16 * s, 1))
    return xs


def kernel(
    ints, dbl, eps_occ_in, eps_virt_in, triple_in, order_in, amp_out, grad_out,
    eps_occ, eps_virt, triple, order,
    kf, fi, g_all, kh, kl, ph, plo, ih, il, s2, s3, r2, r3, t2, first, amp, ev, eb,
    part, c0, q0, xr, q1, yr, q2, zr, q3, fr,
    load_sem, zs, zr_sem, ys, yr_sem, xs, xr_sem, cs, cr_sem, as2, ar2, as3, ar3, out_sem,
    ps, pr, gxs, gxr, gys, gyr, gzs, gzr, gfs, gfr,
):
    vb = lax.axis_index("vb")
    vc = lax.axis_index("vc")
    x, z = vb // 8, vb % 8
    h, y, k = vc // 16, (vc // 2) % 8, vc % 2
    other = 1 - k

    def dev(x_=x, z_=z, h_=h, y_=y, k_=k):
        return (x_ * 8 + z_, h_ * 16 + y_ * 2 + k_)

    def send(src, dst, s_sem, r_sem, to):
        pltpu.make_async_remote_copy(
            src_ref=src, dst_ref=dst, send_sem=s_sem, recv_sem=r_sem, device_id=to, device_id_type=MESH
        ).start()

    def drain(ref, sem):
        pltpu.make_async_copy(ref, ref, sem).wait()

    loads = []
    for l in range(4):
        loads.append(pltpu.make_async_copy(ints.at[0, :, pl.ds(128 * l, 128)], kf.at[l], load_sem.at[1]))
        loads.append(pltpu.make_async_copy(ints.at[1, :, pl.ds(128 * l, 128)], fi.at[l], load_sem.at[2]))
    yt, yl = y // 4, y % 4
    mine = z // 4 == k

    @pl.when(mine)
    def _():
        rows = pl.ds(pl.multiple_of(8 * yt, 8), 8)
        cols = pl.ds(pl.multiple_of(128 * yl, 128), 128)
        for m in range(3):
            pltpu.make_async_copy(dbl.at[m, rows, cols], g_all.at[m, vb, yt, yl], load_sem.at[0]).start()

    small = [(eps_occ_in, eps_occ), (eps_virt_in, eps_virt), (triple_in, triple), (order_in, order)]

    barrier = pltpu.get_barrier_semaphore()

    for j in range(1, 32):
        pl.semaphore_signal(barrier, inc=1, device_id=(lax.rem(vb + j, 32), vc), device_id_type=MESH)
        pl.semaphore_signal(barrier, inc=1, device_id=(vb, lax.rem(vc + j, 32)), device_id_type=MESH)
    for j in range(1, 8):
        pl.semaphore_signal(
            barrier, inc=1, device_id=dev(z_=(z + j) % 8, h_=1 - h), device_id_type=MESH
        )
    for copy in loads:
        copy.start()
    for i, (src, dst) in enumerate(small):
        pltpu.make_async_copy(src, dst, load_sem.at[3 + i]).start()
    pl.semaphore_wait(barrier, 69)

    @pl.when(mine)
    def _():
        drain(g_all.at[0:3, vb, yt, yl], load_sem.at[0])
        for m in (2, 1, 0):
            for j in range(1, 8):
                to = (z + j) % 8
                near = jnp.abs(to - z) <= 4
                send(
                    g_all.at[m, vb, yt, yl], g_all.at[m, vb, yt, yl],
                    zs.at[m], zr_sem.at[m], dev(z_=to, h_=jnp.where(near, h, 1 - h)),
                )

    drain(kf, load_sem.at[1])
    for l in range(4):
        cols = pl.ds(128 * l, 128)
        high, low = halves(kf[l])
        kh[:, cols] = high
        kl[:, cols] = low
        for c in range(16):
            high, low = halves(kf[l, pl.ds(c, 16, stride=16), :])
            ph[pl.ds(16 * c, 16), cols] = high
            plo[pl.ds(16 * c, 16), cols] = low
    drain(fi, load_sem.at[2])
    for l in range(4):
        cols = pl.ds(128 * l, 128)
        high, low = halves(fi[l])
        ih[:, cols] = high
        il[:, cols] = low

    half = 8 * x + 4 * k
    for m in (2, 1, 0):
        @pl.when(mine)
        def _():
            drain(g_all.at[m, 0, 0, pl.ds(0, 3)], zr_sem.at[m])

        @pl.when(jnp.logical_not(mine))
        def _():
            drain(g_all.at[m, 0, 0], zr_sem.at[m])

        block = g_all.at[m, pl.ds(half, 4), yt, yl]
        for j in range(1, 8):
            send(block, block, ys.at[m], yr_sem.at[m], dev(y_=(y + j) % 8))

    def spread(m):
        drain(g_all.at[0, pl.ds(0, 7), 0], yr_sem.at[m])
        block = g_all.at[m, pl.ds(half, 4)]
        send(block, block, cs.at[m], cr_sem.at[m, x], dev(k_=other))
        for j in (1, 3, 2):
            send(block, block, xs.at[m], xr_sem.at[m, x], dev(x_=(x + j) % 4))

    def forward(m, j):
        xg = (x + j) % 4
        block = g_all.at[m, pl.ds(8 * xg + 4 * k, 4)]
        drain(block, xr_sem.at[m, xg])
        send(block, block, cs.at[m], cr_sem.at[m, xg], dev(k_=other))

    def rows_of(m, j):
        xg = (x + j) % 4
        drain(g_all.at[m, pl.ds(8 * xg + 4 * other, 4)], cr_sem.at[m, xg])
        tiles = g_all.at[m, pl.ds(8 * xg, 8)]
        high, low = halves(
            jnp.concatenate([tiles[:, :, l].reshape(128, 128) for l in range(4)], axis=1)
        )
        return xg, high, low

    def third(j):
        xg, dh, dl = rows_of(2, j)
        s3[pl.ds(8 * xg, 8)] = dot3(dh, dl, ih[...], il[...], NT).reshape(8, 16, 256)

        def give(i, carry):
            to = 8 * xg + (i + vc) % 8

            @pl.when(to == vc)
            def _():
                r3[vc] = s3[vc]

            @pl.when(to != vc)
            def _():
                send(s3.at[to], r3.at[vc], as3, ar3.at[vc // 8], (vb, to))

            return carry

        lax.fori_loop(0, 8, give, 0)

    def second(j):
        xg, dh, dl = rows_of(1, j)
        s2[pl.ds(8 * xg, 8)] = dot3(dh, dl, ph[...], plo[...], NT).reshape(8, 16, 256)

        def give(i, carry):
            to = 8 * xg + (i + vb + 4) % 8

            @pl.when(to == vb)
            def _():
                r2[vb] = s2[vb]

            @pl.when(to != vb)
            def _():
                send(s2.at[to], r2.at[vb], as2, ar2.at[x], (to, vc))

            return carry

        lax.fori_loop(0, 8, give, 0)

    def first_term(j):
        xg, dh, dl = rows_of(0, j)
        first[xg] = dot3(kh[...], kl[...], dh, dl, NT)

    spread(2)
    spread(1)
    third(0)
    spread(0)
    forward(2, 1)
    forward(2, 3)
    third(1)
    third(3)
    forward(2, 2)
    forward(1, 1)
    third(2)
    forward(1, 3)
    second(1)
    forward(1, 2)
    second(3)
    forward(0, 1)
    forward(0, 3)
    second(2)
    forward(0, 2)
    second(0)
    for j in (0, 1, 3, 2):
        first_term(j)

    for i, (_, dst) in enumerate(small):
        drain(dst, load_sem.at[3 + i])
    hot = lax.broadcasted_iota(jnp.int32, (V, V), 0) == order[...]
    e_high, e_low = halves(jnp.broadcast_to(eps_virt[...], (8, V)))
    e_rest = (jnp.broadcast_to(eps_virt[...], (8, V)) - e_high.astype(F32) - e_low.astype(F32)).astype(BF16)
    hot = jnp.where(hot, F32(1.0), F32(0.0)).astype(BF16)
    energy = sum(lax.dot_general(e, hot, NN, preferred_element_type=F32) for e in (e_rest, e_low, e_high))[0:1]
    for l in range(4):
        ev[l] = energy[:, 128 * l : 128 * l + 128]
    row = lax.broadcasted_iota(jnp.int32, (256, V), 0)
    col = lax.broadcasted_iota(jnp.int32, (256, V), 1)
    picked = jnp.where(col == 16 * vb + row // 16, energy, F32(0.0))
    b_energy = jnp.sum(picked, axis=1, keepdims=True)
    picked = jnp.where(col == 16 * vc + row % 16, energy, F32(0.0))
    c_energy = jnp.sum(picked, axis=1, keepdims=True)
    place = lax.broadcasted_iota(jnp.int32, (1, NOCC), 1)
    occ = sum(
        jnp.sum(jnp.where(place == triple[:, i : i + 1], eps_occ[...], F32(0.0)), axis=1, keepdims=True)
        for i in range(3)
    )
    eb[...] = jnp.broadcast_to(occ - b_energy - c_energy, (256, 128))

    lane = lax.broadcasted_iota(jnp.int32, (8, 128), 1)

    def group(j):
        g = (x + j) % 4

        @pl.when(g == vc // 8)
        def _():
            drain(s3.at[pl.ds(0, 7)], ar3.at[g])

        @pl.when(g != vc // 8)
        def _():
            drain(s3.at[pl.ds(0, 8)], ar3.at[g])

        for ct in range(2):
            for bh in range(2):
                ws = [r3[8 * g + i, 8 * ct : 8 * ct + 8, 128 * bh : 128 * bh + 128] for i in range(8)]
                for i, w in enumerate(swap_granules(ws, lane)):
                    at = pl.ds((8 * bh + i) * 16 + 8 * ct, 8)
                    first[g, at] = first[g, at] + w
        drain(s2.at[pl.ds(0, 8 if j else 7)], ar2.at[g])
        for bt in range(2):
            for ch in range(2):
                ws = [r2[8 * g + i, 8 * bt : 8 * bt + 8, 128 * ch : 128 * ch + 128] for i in range(8)]
                for i, w in enumerate(swap_granules(ws, lane)):
                    t2[j, pl.ds(128 * bt + 8 * ch + i, 8, stride=16), :] = w
        total = (first[g] + t2[j]) / (eb[...] - ev[g])
        amp[j] = total
        th, tl = halves(total.T)
        part[pl.ds(8 * g, 8)] = dot3(th, tl, kh[...], kl[...], NN).reshape(8, 2, 8, V)
        send(part.at[pl.ds(8 * g, 8), other], c0.at[pl.ds(8 * g, 8)], ps, pr.at[g], dev(k_=other))
        pltpu.make_async_copy(
            amp.at[j], amp_out.at[:, pl.ds(pl.multiple_of(128 * g, 128), 128)], out_sem
        ).start()

    def over_cores(j):
        g = (x + j) % 4
        block = pl.ds(8 * g, 8)
        drain(c0.at[block], pr.at[g])
        q0[block] = part[block, k] + c0[block]
        if j:
            send(q0.at[block], xr.at[j - 1], gxs, gxr, dev(x_=g))

    group(3)
    group(1)
    over_cores(3)
    group(2)
    over_cores(1)
    over_cores(2)
    group(0)
    over_cores(0)
    drain(xr, gxr)
    q1[...] = (q0[pl.ds(8 * x, 8)] + xr[0]) + (xr[1] + xr[2])
    for j in range(1, 8):
        send(q1.at[(y + j) % 8], yr.at[j - 1], gys, gyr, dev(y_=(y + j) % 8))
    drain(yr, gyr)
    rows = q1[y] + jnp.sum(yr[...], axis=0)
    q2[0] = rows[:, 0:256]
    q2[1] = rows[:, 256:512]
    for hh in range(2):
        here = jnp.logical_and(z == y, h == hh)

        @pl.when(here)
        def _():
            zr[8 * h + z] = q2[hh]

        @pl.when(jnp.logical_not(here))
        def _():
            send(q2.at[hh], zr.at[8 * h + z], gzs.at[hh], gzr, dev(z_=y, h_=hh))

    @pl.when(z == y)
    def _():
        drain(zr.at[pl.ds(0, 15)], gzr)
        total = jnp.sum(zr[...], axis=0)
        q3[0] = total[:, 0:128]
        q3[1] = total[:, 128:256]

        def give(i, carry):
            @pl.when(16 * h + i == vc)
            def _():
                fr[k] = q3[i // 8]

            @pl.when(16 * h + i != vc)
            def _():
                send(q3.at[i // 8], fr.at[k], gfs, gfr.at[k], (vb, 16 * h + i))

            return carry

        lax.fori_loop(0, 16, give, 0)

    for r in range(2):
        @pl.when(jnp.logical_or(z != y, k != r))
        def _():
            drain(fr.at[r], gfr.at[r])

    place = vc % 8
    for r in range(2):
        got = fr[r]
        mine_cols = got[:, 0:16]
        for i in range(1, 8):
            mine_cols = jnp.where(place == i, got[:, 16 * i : 16 * i + 16], mine_cols)
        grad_out[8 * r : 8 * r + 8, :] = mine_cols

    @pl.when(mine)
    def _():
        for m in range(3):
            drain(g_all.at[m, pl.ds(0, 7), 0, 0], zs.at[m])

    for m in range(3):
        drain(g_all.at[0, pl.ds(0, 7), 0], ys.at[m])
        drain(g_all.at[m, pl.ds(0, 12)], xs.at[m])
        drain(g_all.at[m, pl.ds(0, 16)], cs.at[m])
    drain(s3.at[pl.ds(0, 31)], as3)
    drain(s2.at[pl.ds(0, 31)], as2)
    drain(c0, ps)
    drain(xr, gxs)
    drain(yr, gys)
    for hh in range(2):
        @pl.when(jnp.logical_not(jnp.logical_and(z == y, h == hh)))
        def _():
            drain(q2.at[hh], gzs.at[hh])

    @pl.when(z == y)
    def _():
        drain(t2.at[0, pl.ds(0, 120)], gfs)

    drain(amp, out_sem)


def on_device(integrals, doubles, eps_occ, eps_virt, triple, energy_order):
    vmem = pl.BlockSpec(memory_space=pltpu.VMEM)
    anyw = pl.BlockSpec(memory_space=pl.ANY)
    dma = pltpu.SemaphoreType.DMA
    f = lambda *s: pltpu.VMEM(s, F32)
    b = lambda *s: pltpu.VMEM(s, BF16)
    amp, grad = pl.pallas_call(
        kernel,
        out_shape=(jax.ShapeDtypeStruct((256, V), F32), jax.ShapeDtypeStruct((16, 16), F32)),
        in_specs=[anyw] * 6,
        out_specs=(anyw, vmem),
        scratch_shapes=[
            f(1, NOCC), f(1, V), pltpu.VMEM((1, 3), jnp.int32), pltpu.VMEM((1, V), jnp.int32),
            f(4, 256, 128), f(4, 256, 128), f(3, 32, 2, 4, 8, 128),
            b(256, V), b(256, V), b(256, V), b(256, V), b(256, V), b(256, V),
            f(32, 16, 256), f(32, 16, 256), f(32, 16, 256), f(32, 16, 256),
            f(4, 256, 128), f(4, 256, 128), f(4, 256, 128), f(4, 1, 128), f(256, 128),
            f(32, 2, 8, V), f(32, 8, V), f(32, 8, V), f(3, 8, 8, V), f(8, 8, V), f(7, 8, V),
            f(2, 8, 256), f(16, 8, 256), f(2, 8, 128), f(2, 8, 128),
            dma((7,)), dma((3,)), dma((3,)), dma((3,)), dma((3,)), dma((3,)), dma((3, 4)), dma((3,)), dma((3, 4)),
            dma, dma((4,)), dma, dma((4,)), dma,
            dma, dma((4,)), dma, dma, dma, dma, dma((2,)), dma, dma, dma((2,)),
        ],
        compiler_params=pltpu.CompilerParams(
            collective_id=0, has_side_effects=True, vmem_limit_bytes=60 * 1024 * 1024
        ),
    )(
        integrals.reshape(2, 256, V),
        doubles,
        eps_occ.reshape(1, NOCC),
        eps_virt.reshape(1, V),
        triple.reshape(1, 3),
        energy_order.reshape(1, V),
    )
    return amp.reshape(16, 16, V), grad


def solution(mesh):
    return jax.shard_map(
        on_device,
        mesh=mesh,
        in_specs=(P(None, "vb", "vc", None), P(None, "vb", None), P(), P(), P(), P()),
        out_specs=(P("vb", "vc", None), P("vb", "vc")),
        check_vma=False,
    )
```

```python
import jax
import jax.numpy as jnp
from jax import lax
from jax.experimental import pallas as pl
from jax.experimental.pallas import tpu as pltpu
from jax.sharding import PartitionSpec as P

V = 512
NOCC = 100
MESH = pl.DeviceIdType.MESH
F32 = jnp.float32
BF16 = jnp.bfloat16
NT = (((1,), (1,)), ((), ()))
NN = (((1,), (0,)), ((), ()))


def halves(x):
    high = x.astype(BF16)
    return high, (x - high.astype(F32)).astype(BF16)


def dot3(ah, al, bh, bl, dims):
    def one(a, b):
        return lax.dot_general(a, b, dims, preferred_element_type=F32)

    return one(ah, bh) + (one(ah, bl) + one(al, bh))


def swap_granules(xs, lane):
    xs = list(xs)
    for s in (1, 2, 4):
        upper = (lane & (16 * s)) != 0
        for i in range(8):
            if i & s == 0:
                a, b = xs[i], xs[i + s]
                xs[i] = jnp.where(upper, pltpu.roll(b, 16 * s, 1), a)
                xs[i + s] = jnp.where(upper, b, pltpu.roll(a, 128 - 16 * s, 1))
    return xs


def kernel(
    ints, dbl, eps_occ_in, eps_virt_in, triple_in, order_in, amp_out, grad_out,
    eps_occ, eps_virt, triple, order,
    kf, fi, g_all, kh, kl, ph, plo, ih, il, s2, s3, r2, r3, t2, first, amp, ev, eb,
    part, c0, q0, xr, q1, q2, zr, fr,
    load_sem, zs, zr_sem, ys, yr_sem, xs, xr_sem, cs, cr_sem, as2, ar2, as3, ar3, out_sem,
    ps, pr, gxs, gxr, gzs, gzr, gfs, gfr, far_sem,
):
    vb = lax.axis_index("vb")
    vc = lax.axis_index("vc")
    x, z = vb // 8, vb % 8
    h, y, k = vc // 16, (vc // 2) % 8, vc % 2
    other = 1 - k

    def dev(x_=x, z_=z, h_=h, y_=y, k_=k):
        return (x_ * 8 + z_, h_ * 16 + y_ * 2 + k_)

    def send(src, dst, s_sem, r_sem, to):
        pltpu.make_async_remote_copy(
            src_ref=src, dst_ref=dst, send_sem=s_sem, recv_sem=r_sem, device_id=to, device_id_type=MESH
        ).start()

    def drain(ref, sem):
        pltpu.make_async_copy(ref, ref, sem).wait()

    loads = []
    for l in range(4):
        loads.append(pltpu.make_async_copy(ints.at[0, :, pl.ds(128 * l, 128)], kf.at[l], load_sem.at[1]))
        loads.append(pltpu.make_async_copy(ints.at[1, :, pl.ds(128 * l, 128)], fi.at[l], load_sem.at[2]))
    yt, yl = y // 4, y % 4
    mine = z // 4 == k

    @pl.when(mine)
    def _():
        rows = pl.ds(pl.multiple_of(8 * yt, 8), 8)
        cols = pl.ds(pl.multiple_of(128 * yl, 128), 128)
        for m in range(3):
            pltpu.make_async_copy(dbl.at[m, rows, cols], g_all.at[m, vb, yt, yl], load_sem.at[0]).start()

    small = [(eps_occ_in, eps_occ), (eps_virt_in, eps_virt), (triple_in, triple), (order_in, order)]

    barrier = pltpu.get_barrier_semaphore()

    far = [(vb, 16 * (1 - h) + i) for i in range(16)]
    far += [dev(z_=lax.rem(z + j, 8), h_=1 - h) for j in range(1, 8)]
    for j in range(1, 32):
        pl.semaphore_signal(barrier, inc=1, device_id=(lax.rem(vb + j, 32), vc), device_id_type=MESH)
    for j in range(1, 16):
        to = 16 * h + lax.rem(vc % 16 + j, 16)
        pl.semaphore_signal(barrier, inc=1, device_id=(vb, to), device_id_type=MESH)

    @pl.when(h == 0)
    def _():
        for to in far:
            pl.semaphore_signal(barrier, inc=1, device_id=to, device_id_type=MESH)

    for copy in loads:
        copy.start()
    for i, (src, dst) in enumerate(small):
        pltpu.make_async_copy(src, dst, load_sem.at[3 + i]).start()
    pl.semaphore_wait(barrier, 46 + 23 * h)

    @pl.when(h == 1)
    def _():
        for to in far:
            pl.semaphore_signal(far_sem, inc=1, device_id=to, device_id_type=MESH)


    @pl.when(mine)
    def _():
        drain(g_all.at[0:3, vb, yt, yl], load_sem.at[0])
        for m in (2, 1, 0):
            for j in range(1, 8):
                to = (z + j) % 8
                send(
                    g_all.at[m, vb, yt, yl], g_all.at[m, vb, yt, yl],
                    zs.at[m], zr_sem.at[m], dev(z_=to),
                )

    drain(kf, load_sem.at[1])
    for l in range(4):
        cols = pl.ds(128 * l, 128)
        high, low = halves(kf[l])
        kh[:, cols] = high
        kl[:, cols] = low
        for c in range(16):
            high, low = halves(kf[l, pl.ds(c, 16, stride=16), :])
            ph[pl.ds(16 * c, 16), cols] = high
            plo[pl.ds(16 * c, 16), cols] = low
    drain(fi, load_sem.at[2])
    for l in range(4):
        cols = pl.ds(128 * l, 128)
        high, low = halves(fi[l])
        ih[:, cols] = high
        il[:, cols] = low

    half = 8 * x + 4 * k
    for m in (2, 1, 0):
        @pl.when(mine)
        def _():
            drain(g_all.at[m, 0, 0, pl.ds(0, 3)], zr_sem.at[m])

        @pl.when(jnp.logical_not(mine))
        def _():
            drain(g_all.at[m, 0, 0], zr_sem.at[m])

        block = g_all.at[m, pl.ds(half, 4), yt, yl]
        for j in range(1, 8):
            send(block, block, ys.at[m], yr_sem.at[m], dev(y_=(y + j) % 8))

    def spread(m):
        drain(g_all.at[0, pl.ds(0, 7), 0], yr_sem.at[m])
        block = g_all.at[m, pl.ds(half, 4)]
        send(block, block, cs.at[m], cr_sem.at[m, x], dev(k_=other))
        for j in (1, 3, 2):
            send(block, block, xs.at[m], xr_sem.at[m, x], dev(x_=(x + j) % 4))

    def forward(m, j):
        xg = (x + j) % 4
        block = g_all.at[m, pl.ds(8 * xg + 4 * k, 4)]
        drain(block, xr_sem.at[m, xg])
        send(block, block, cs.at[m], cr_sem.at[m, xg], dev(k_=other))

    def rows_of(m, j):
        xg = (x + j) % 4
        drain(g_all.at[m, pl.ds(8 * xg + 4 * other, 4)], cr_sem.at[m, xg])
        tiles = g_all.at[m, pl.ds(8 * xg, 8)]
        high, low = halves(
            jnp.concatenate([tiles[:, :, l].reshape(128, 128) for l in range(4)], axis=1)
        )
        return xg, high, low

    def third(j):
        xg, dh, dl = rows_of(2, j)
        s3[pl.ds(8 * xg, 8)] = dot3(dh, dl, ih[...], il[...], NT).reshape(8, 16, 256)

        def give(i, carry):
            to = 8 * xg + (i + vc) % 8

            @pl.when(to == vc)
            def _():
                r3[vc] = s3[vc]

            @pl.when(to != vc)
            def _():
                send(s3.at[to], r3.at[vc], as3, ar3.at[vc // 8], (vb, to))

            return carry

        lax.fori_loop(0, 8, give, 0)

    def second(j):
        xg, dh, dl = rows_of(1, j)
        s2[pl.ds(8 * xg, 8)] = dot3(dh, dl, ph[...], plo[...], NT).reshape(8, 16, 256)

        def give(i, carry):
            to = 8 * xg + (i + vb + 4) % 8

            @pl.when(to == vb)
            def _():
                r2[vb] = s2[vb]

            @pl.when(to != vb)
            def _():
                send(s2.at[to], r2.at[vb], as2, ar2.at[x], (to, vc))

            return carry

        lax.fori_loop(0, 8, give, 0)

    def first_term(j):
        xg, dh, dl = rows_of(0, j)
        first[xg] = dot3(kh[...], kl[...], dh, dl, NT)

    spread(2)
    spread(1)

    @pl.when(h == 0)
    def _():
        pl.semaphore_wait(far_sem, 23)

    third(0)
    spread(0)
    forward(2, 1)
    forward(2, 3)
    third(1)
    third(3)
    forward(2, 2)
    forward(1, 1)
    third(2)
    forward(1, 3)
    second(1)
    forward(1, 2)
    second(3)
    forward(0, 1)
    forward(0, 3)
    second(2)
    forward(0, 2)
    second(0)
    for j in (0, 1, 3, 2):
        first_term(j)

    for i, (_, dst) in enumerate(small):
        drain(dst, load_sem.at[3 + i])
    hot = lax.broadcasted_iota(jnp.int32, (V, V), 0) == order[...]
    e_high, e_low = halves(jnp.broadcast_to(eps_virt[...], (8, V)))
    e_rest = (jnp.broadcast_to(eps_virt[...], (8, V)) - e_high.astype(F32) - e_low.astype(F32)).astype(BF16)
    hot = jnp.where(hot, F32(1.0), F32(0.0)).astype(BF16)
    energy = sum(lax.dot_general(e, hot, NN, preferred_element_type=F32) for e in (e_rest, e_low, e_high))[0:1]
    for l in range(4):
        ev[l] = energy[:, 128 * l : 128 * l + 128]
    row = lax.broadcasted_iota(jnp.int32, (256, V), 0)
    col = lax.broadcasted_iota(jnp.int32, (256, V), 1)
    picked = jnp.where(col == 16 * vb + row // 16, energy, F32(0.0))
    b_energy = jnp.sum(picked, axis=1, keepdims=True)
    picked = jnp.where(col == 16 * vc + row % 16, energy, F32(0.0))
    c_energy = jnp.sum(picked, axis=1, keepdims=True)
    place = lax.broadcasted_iota(jnp.int32, (1, NOCC), 1)
    occ = sum(
        jnp.sum(jnp.where(place == triple[:, i : i + 1], eps_occ[...], F32(0.0)), axis=1, keepdims=True)
        for i in range(3)
    )
    eb[...] = jnp.broadcast_to(occ - b_energy - c_energy, (256, 128))

    lane = lax.broadcasted_iota(jnp.int32, (8, 128), 1)

    def group(j):
        g = (x + j) % 4

        @pl.when(g == vc // 8)
        def _():
            drain(s3.at[pl.ds(0, 7)], ar3.at[g])

        @pl.when(g != vc // 8)
        def _():
            drain(s3.at[pl.ds(0, 8)], ar3.at[g])

        for ct in range(2):
            for bh in range(2):
                ws = [r3[8 * g + i, 8 * ct : 8 * ct + 8, 128 * bh : 128 * bh + 128] for i in range(8)]
                for i, w in enumerate(swap_granules(ws, lane)):
                    at = pl.ds((8 * bh + i) * 16 + 8 * ct, 8)
                    first[g, at] = first[g, at] + w
        drain(s2.at[pl.ds(0, 8 if j else 7)], ar2.at[g])
        for bt in range(2):
            for ch in range(2):
                ws = [r2[8 * g + i, 8 * bt : 8 * bt + 8, 128 * ch : 128 * ch + 128] for i in range(8)]
                for i, w in enumerate(swap_granules(ws, lane)):
                    t2[j, pl.ds(128 * bt + 8 * ch + i, 8, stride=16), :] = w
        total = (first[g] + t2[j]) / (eb[...] - ev[g])
        amp[j] = total
        th, tl = halves(total.T)
        part[pl.ds(8 * g, 8)] = dot3(th, tl, kh[...], kl[...], NN).reshape(8, 2, 8, V)
        send(part.at[pl.ds(8 * g, 8), other], c0.at[pl.ds(8 * g, 8)], ps, pr.at[g], dev(k_=other))
        pltpu.make_async_copy(
            amp.at[j], amp_out.at[:, pl.ds(pl.multiple_of(128 * g, 128), 128)], out_sem
        ).start()

    def over_cores(j):
        g = (x + j) % 4
        block = pl.ds(8 * g, 8)
        drain(c0.at[block], pr.at[g])
        q0[block] = part[block, k] + c0[block]
        if j:
            send(q0.at[block], xr.at[j - 1], gxs, gxr, dev(x_=g))

    group(3)
    group(1)
    over_cores(3)
    group(2)
    over_cores(1)
    over_cores(2)
    group(0)
    over_cores(0)
    drain(xr, gxr)
    rows = (q0[pl.ds(8 * x, 8)] + xr[0]) + (xr[1] + xr[2])
    q1[0] = rows[:, :, 0:256]
    q1[1] = rows[:, :, 256:512]
    for o in (8, 7, 9, 6, 10, 5, 11, 4, 12, 3, 13, 2, 14, 1, 15):
        to = lax.rem(8 * h + z + o, 16)
        send(q1.at[to // 8, to % 8], zr.at[8 * h + z], gzs, gzr, dev(z_=to % 8, h_=to // 8))
    zr[8 * h + z] = q1[h, z]
    drain(zr.at[pl.ds(0, 15)], gzr)
    total = jnp.sum(zr[...], axis=0)
    q2[0] = total[:, 0:128]
    q2[1] = total[:, 128:256]
    for o in (8, 9, 7, 6, 10, 5, 11, 4, 12, 3, 13, 2, 14, 1, 15):
        to = lax.rem(vc % 16 + o, 16)
        send(q2.at[to // 8], fr.at[vc % 16], gfs, gfr, (vb, 16 * h + to))
    fr[vc % 16] = q2[(vc % 16) // 8]
    drain(fr.at[pl.ds(0, 15)], gfr)
    place = vc % 8
    for r in range(2):
        got = sum(fr[2 * i + r] for i in range(8))
        mine_cols = got[:, 0:16]
        for i in range(1, 8):
            mine_cols = jnp.where(place == i, got[:, 16 * i : 16 * i + 16], mine_cols)
        grad_out[8 * r : 8 * r + 8, :] = mine_cols

    @pl.when(mine)
    def _():
        for m in range(3):
            drain(g_all.at[m, pl.ds(0, 7), 0, 0], zs.at[m])

    for m in range(3):
        drain(g_all.at[0, pl.ds(0, 7), 0], ys.at[m])
        drain(g_all.at[m, pl.ds(0, 12)], xs.at[m])
        drain(g_all.at[m, pl.ds(0, 16)], cs.at[m])
    drain(s3.at[pl.ds(0, 31)], as3)
    drain(s2.at[pl.ds(0, 31)], as2)
    drain(c0, ps)
    drain(xr, gxs)
    drain(zr.at[pl.ds(0, 15)], gzs)
    drain(fr.at[pl.ds(0, 15)], gfs)
    drain(amp, out_sem)


def on_device(integrals, doubles, eps_occ, eps_virt, triple, energy_order):
    vmem = pl.BlockSpec(memory_space=pltpu.VMEM)
    anyw = pl.BlockSpec(memory_space=pl.ANY)
    dma = pltpu.SemaphoreType.DMA
    f = lambda *s: pltpu.VMEM(s, F32)
    b = lambda *s: pltpu.VMEM(s, BF16)
    amp, grad = pl.pallas_call(
        kernel,
        out_shape=(jax.ShapeDtypeStruct((256, V), F32), jax.ShapeDtypeStruct((16, 16), F32)),
        in_specs=[anyw] * 6,
        out_specs=(anyw, vmem),
        scratch_shapes=[
            f(1, NOCC), f(1, V), pltpu.VMEM((1, 3), jnp.int32), pltpu.VMEM((1, V), jnp.int32),
            f(4, 256, 128), f(4, 256, 128), f(3, 32, 2, 4, 8, 128),
            b(256, V), b(256, V), b(256, V), b(256, V), b(256, V), b(256, V),
            f(32, 16, 256), f(32, 16, 256), f(32, 16, 256), f(32, 16, 256),
            f(4, 256, 128), f(4, 256, 128), f(4, 256, 128), f(4, 1, 128), f(256, 128),
            f(32, 2, 8, V), f(32, 8, V), f(32, 8, V), f(3, 8, 8, V), f(2, 8, 8, 256),
            f(2, 8, 128), f(16, 8, 256), f(16, 8, 128),
            dma((7,)), dma((3,)), dma((3,)), dma((3,)), dma((3,)), dma((3,)), dma((3, 4)), dma((3,)), dma((3, 4)),
            dma, dma((4,)), dma, dma((4,)), dma,
            dma, dma((4,)), dma, dma, dma, dma, dma, dma,
            pltpu.SemaphoreType.REGULAR,
        ],
        compiler_params=pltpu.CompilerParams(
            collective_id=0, has_side_effects=True, vmem_limit_bytes=60 * 1024 * 1024
        ),
    )(
        integrals.reshape(2, 256, V),
        doubles,
        eps_occ.reshape(1, NOCC),
        eps_virt.reshape(1, V),
        triple.reshape(1, 3),
        energy_order.reshape(1, V),
    )
    return amp.reshape(16, 16, V), grad


def solution(mesh):
    return jax.shard_map(
        on_device,
        mesh=mesh,
        in_specs=(P(None, "vb", "vc", None), P(None, "vb", None), P(), P(), P(), P()),
        out_specs=(P("vb", "vc", None), P("vb", "vc")),
        check_vma=False,
    )
```
